256 devices in a mesh: groups: 2 (over y), ep: 16 (over z), dp: 4 (over x), tp: 2 (over core).
Axes of the slice: x: 4, y: 2, z: 16, core: 2. Of those that a mesh axis runs over, the one named last changes fastest.
The devices are a block of a 4x16x16 slice.
Arguments:
- tokens: bfloat16 [16384, 2048], P(('groups', 'ep', 'dp', 'tp')), parts along dimension 0, may hold values from -6 to 6
- experts_one: int32 [16384, 8], P(('groups', 'ep', 'dp', 'tp')), parts along dimension 0, may hold values from 0 to 63, all different within a row; in each aligned block of 64 rows (0 to 63, 64 to 127, ...) at most 10 rows name the same one
- gates_one: float32 [16384, 8], P(('groups', 'ep', 'dp', 'tp')), parts along dimension 0, may hold values from 0.05 to 0.5
- w_in_one: bfloat16 [64, 2048, 2, 768], P(('ep', 'dp'), None, None, 'tp'), may hold values from -0.125 to 0.125
- w_down_one: bfloat16 [64, 768, 2048], P(('ep', 'dp'), 'tp'), may hold values from -0.21875 to 0.21875
- norm_gain: float32 [2048], replicated, may hold values from 0.5 to 1.5
- experts_two: int32 [16384, 8], P(('groups', 'ep', 'dp', 'tp')), parts along dimension 0, may hold values from 0 to 63, all different within a row; in each aligned block of 64 rows (0 to 63, 64 to 127, ...) at most 10 rows name the same one
- gates_two: float32 [16384, 8], P(('groups', 'ep', 'dp', 'tp')), parts along dimension 0, may hold values from 0.05 to 0.5
- placement_two: int32 [64], replicated, may hold values from 0 to 63, each once
- w_in_two: bfloat16 [64, 2048, 2, 768], P(('ep', 'dp'), None, None, 'tp'), may hold values from -0.125 to 0.125
- w_down_two: bfloat16 [64, 768, 2048], P(('ep', 'dp'), 'tp'), may hold values from -0.21875 to 0.21875
Outputs:
- layer_out: bfloat16 [16384, 2048], P(('groups', 'ep', 'dp', 'tp')), parts along dimension 0
The draws below stay inside these ranges and needn't reach their ends.
There are 2 independent parts, one for each index of `groups`. The reference program is written for one: setup_inputs(seed, part) draws one part's arguments, and reference() takes and returns one part's arrays. A program takes and returns all parts, laid end to end along the dimension named above; an argument that names none is the same for every part. Nothing has to cross between parts.
Inputs may be any that keep to these rules, and one draw needn't show every extreme that they name: `experts_one`: each token names 8 different experts; among the 64 tokens of one device no expert is named more than 10 times, and on some device some expert is named exactly 10 times. `experts_two`: each token names 8 different experts; among the 64 tokens of one device no expert is named more than 10 times, and on some device some expert is named exactly 10 times. `placement_two`: each slot is named by exactly one expert.
All inputs are finite; a program needn't handle non-finite values.
Results may differ from the reference program's by a relative error of at most 0.011.
Values may be sent and summed in bfloat16 or wider, within the bound.
A program may use at most 128 MiB of HBM per device.

```python
import math
import jax
import jax.numpy as jnp
import numpy as np
from jax import lax

D = 2048
FF = 768
TOPK = 8
TOK_DEV = 64
EXPERTS = 64
MOST = 10
TOKENS = 8192
N_EP = 16
N_DP = 4
N_TP = 2


def shard_levels(key, dims, cuts, smallest, top_value):
    loudness, own = 1.0, jax.random.fold_in(key, 6)
    for position, parts in cuts:
        heights = jnp.exp(jax.random.uniform(jax.random.fold_in(own, position), (parts,), jnp.float32, smallest / len(cuts), top_value / len(cuts)))
        loudness = loudness * jnp.repeat(heights, dims[position] // parts).reshape([-1 if axis == position else 1 for axis in range(len(dims))])
    return loudness


def assign_block(stream_key, own, number, rows, count, top, limit, lean):
    sequence = jax.random.permutation(stream_key, count)
    crowded, common = shares(count, rows * top, limit, lean, True), shares(count, rows * top, limit, lean, False)
    places = jnp.arange(count)

    def named(sizes, rotation):
        used = int((sizes > 0).sum())
        fixed = max(1, used // 4)
        passed = fixed + (places - fixed + rotation * (used - fixed)) % max(1, count - fixed)
        return jnp.zeros((count,), jnp.int32).at[sequence[jnp.where(places < fixed, places, passed)]].set(jnp.asarray(sizes, jnp.int32))

    sizes = jnp.where(number % 4 == 0, named(crowded, number // 4), named(common, number - number // 4 - 1))
    mixed = jax.random.permutation(jax.random.fold_in(own, 3), count)
    giver, receiver = mixed[0:count // 2 * 2:2], mixed[1:count // 2 * 2:2]
    margin = jnp.minimum(sizes[giver] - 1, limit - sizes[receiver]) // 2
    margin = jnp.where((giver == sequence[0]) | (receiver == sequence[0]) | (sizes[receiver] == 0), 0, jnp.maximum(margin, 0))
    passed = jax.random.randint(jax.random.fold_in(own, 4), (count // 2,), 0, 1 << 20) % (margin + 1)
    sizes = sizes.at[giver].add(-passed).at[receiver].add(passed)
    labels = jnp.searchsorted(jnp.cumsum(sizes), jnp.arange(rows * top), side="right").astype(jnp.int32)
    listing = labels.reshape(top, rows).T
    listing = listing[jax.random.permutation(jax.random.fold_in(own, 1), rows)]
    rotation = jax.random.randint(jax.random.fold_in(own, 2), (rows, 1), 0, top)
    return jnp.take_along_axis(listing, (jnp.arange(top)[None, :] + rotation) % top, axis=1)


def shares(count, total, bound, lean, full):
    weights = [(1 << 20) // math.isqrt(rank ** lean) + 1 for rank in range(1, count + 1)]
    largest = bound if full else min(bound, max(-(-total // count), total * weights[0] // sum(weights)))
    least = 1 if total - largest >= count - 1 else 0
    holding, spare = [largest] + [least] * (count - 1), total - largest - least * (count - 1)
    while spare > 0:
        candidates = [i for i in range(1, count) if holding[i] < largest] or [i for i in range(1, count) if holding[i] < bound]
        whole, remaining = sum([weights[i] for i in candidates]), spare
        for i in candidates:
            more = min(bound - holding[i], max(1, remaining * weights[i] // whole), spare)
            holding[i] = holding[i] + more
            spare = spare - more
    return np.array(holding)


def gaussian(own_key, extent, scale, reach, cuts=(), kind=jnp.bfloat16):
    entries = jax.random.normal(own_key, extent, jnp.float32) * scale
    if len(cuts) > 0:
        entries = shard_levels(own_key, extent, cuts, -0.22, 0.18) * entries
    return jnp.clip(entries, min=-reach, max=reach).astype(kind)


def setup_inputs(seed: int = 0, part: int = 0) -> dict:
    key_of = jax.random.split(jax.random.key(seed), 12)
    part_splits = jax.random.split(jax.random.fold_in(key_of[11], part), 12)
    tokens = gaussian(part_splits[0], (TOKENS, D), 1.0, 6.0, ((0, 128),))
    experts_one_keys = jax.random.split(jax.random.fold_in(part_splits[1], 1), TOKENS // TOK_DEV)
    experts_one_turns = jax.random.permutation(jax.random.fold_in(part_splits[1], 3), TOKENS // TOK_DEV)
    experts_one = jax.vmap(lambda own, number: assign_block(jax.random.fold_in(part_splits[1], 2), own, number, TOK_DEV, EXPERTS, TOPK, MOST, 2))(experts_one_keys, experts_one_turns).reshape((TOKENS, TOPK))
    gates_one = jnp.clip(jnp.exp(math.log(0.5) - 2.3025851 * jax.random.uniform(part_splits[2], (TOKENS, TOPK), jnp.float32) ** shard_levels(part_splits[2], (TOKENS, TOPK), ((0, 128),), -0.2, 0.2)), 0.05, 0.5)
    w_in_one = gaussian(key_of[3], (EXPERTS, D, 2, FF), D ** -0.5, 0.125, ((0, 64), (3, 2)))
    w_down_one = gaussian(key_of[4], (EXPERTS, FF, D), FF ** -0.5, 0.21875, ((0, 64), (1, 2)))
    norm_gain = jnp.clip(1.0 + 0.1 * jax.random.normal(key_of[5], (D,), jnp.float32), 0.5, 1.5)
    experts_two_keys = jax.random.split(jax.random.fold_in(part_splits[6], 1), TOKENS // TOK_DEV)
    experts_two_turns = jax.random.permutation(jax.random.fold_in(part_splits[6], 3), TOKENS // TOK_DEV)
    experts_two = jax.vmap(lambda own, number: assign_block(jax.random.fold_in(part_splits[6], 2), own, number, TOK_DEV, EXPERTS, TOPK, MOST, 2))(experts_two_keys, experts_two_turns).reshape((TOKENS, TOPK))
    gates_two = jnp.clip(jnp.exp(math.log(0.5) - 2.3025851 * jax.random.uniform(part_splits[7], (TOKENS, TOPK), jnp.float32) ** shard_levels(part_splits[7], (TOKENS, TOPK), ((0, 128),), -0.2, 0.2)), 0.05, 0.5)
    placement_two = jax.random.permutation(key_of[8], EXPERTS).astype(jnp.int32)
    w_in_two = gaussian(key_of[9], (EXPERTS, D, 2, FF), D ** -0.5, 0.125, ((0, 64), (3, 2)))
    w_down_two = gaussian(key_of[10], (EXPERTS, FF, D), FF ** -0.5, 0.21875, ((0, 64), (1, 2)))
    return dict(tokens=tokens, experts_one=experts_one, gates_one=gates_one, w_in_one=w_in_one, w_down_one=w_down_one, norm_gain=norm_gain, experts_two=experts_two, gates_two=gates_two, placement_two=placement_two, w_in_two=w_in_two, w_down_two=w_down_two)


def expert_layer(rows_in, layer_slots, gate_values, w_in, w_down):
    token_count, top_count = layer_slots.shape
    expert_total, row_width, pair_n, hidden_n = w_in.shape
    slot_cap = MOST * N_EP * N_DP * N_TP
    block_width = hidden_n // N_TP
    flat_ids = layer_slots.reshape(-1)
    owner_row = jnp.arange(token_count * top_count, dtype=jnp.int32) // top_count
    flat_gates = gate_values.reshape(-1)

    def accumulate(summed, expert_id):
        hit_mask = flat_ids == expert_id
        slot_rank = jnp.cumsum(hit_mask.astype(jnp.int32)) - 1
        slot_pos = jnp.where(hit_mask, slot_rank, slot_cap).astype(jnp.int32)
        picked = jnp.zeros((slot_cap,), jnp.int32).at[slot_pos].set(owner_row, mode='drop')
        weight = jnp.zeros((slot_cap,), jnp.float32).at[slot_pos].set(flat_gates, mode='drop')
        chosen = rows_in[picked]
        gate_up = jnp.dot(chosen, w_in[expert_id].reshape(row_width, pair_n * hidden_n), preferred_element_type=jnp.float32)
        activated = (jax.nn.silu(gate_up[:, :hidden_n]) * gate_up[:, hidden_n:]).astype(jnp.bfloat16)
        down_now = w_down[expert_id]
        total = jnp.zeros((slot_cap, row_width), jnp.float32)
        for block in range(N_TP):
            lo_unit = block * block_width
            partial_out = jnp.dot(activated[:, lo_unit:lo_unit + block_width], down_now[lo_unit:lo_unit + block_width], preferred_element_type=jnp.float32)
            total = total + partial_out.astype(jnp.bfloat16).astype(jnp.float32)
        expert_out = total.astype(jnp.bfloat16)
        summed = summed.at[picked].add(weight[:, None] * expert_out.astype(jnp.float32))
        return (summed, None)
    start_sum = jnp.zeros((token_count, row_width), jnp.float32)
    summed, _ = lax.scan(accumulate, start_sum, jnp.arange(expert_total, dtype=jnp.int32))
    return summed

def reference(tokens, experts_one, gates_one, w_in_one, w_down_one, norm_gain, experts_two, gates_two, placement_two, w_in_two, w_down_two):
    moe_one = expert_layer(tokens, experts_one, gates_one, w_in_one, w_down_one)
    mixed = (tokens.astype(jnp.float32) + moe_one).astype(jnp.bfloat16)
    mixed = lax.optimization_barrier(mixed)
    mixed_wide = mixed.astype(jnp.float32)
    inv_rms = lax.rsqrt(lax.optimization_barrier(jnp.mean(mixed_wide * mixed_wide, axis=1, keepdims=True)) + 1e-06)
    normed = (mixed_wide * inv_rms * norm_gain[None, :]).astype(jnp.bfloat16)
    layer_slots = placement_two[experts_two].astype(jnp.int32)
    moe_two = expert_layer(normed, layer_slots, gates_two, w_in_two, w_down_two)
    return (mixed_wide + moe_two).astype(jnp.bfloat16)
```

```python
import functools

import jax
import jax.numpy as jnp
from jax import lax
from jax.experimental import pallas as pl
from jax.experimental.pallas import tpu as pltpu
from jax.sharding import PartitionSpec as P

F32, BF16 = jnp.float32, jnp.bfloat16
MESH = pl.DeviceIdType.MESH
PIECES = 4


def capacity(tok_rows, top_count, expert_count):
    return max(2, min(tok_rows, 5 * tok_rows * top_count // (4 * expert_count)))


def layer_kernel(dims, with_norm, *refs):
    nz, nx, tok, width, half_ff, top, cap, rows = dims
    steps = nz // 2
    pr = tok // PIECES
    slab = nx * rows
    refs = list(refs)
    rows_ref, meta_ref, w_in, w_down = refs[:4]
    refs = refs[4:]
    if with_norm:
        gain_ref, mixed_ref, normed_ref = refs[:3]
        resid_ref = rows_ref
        refs = refs[3:]
    else:
        resid_ref, out_ref = refs[:2]
        refs = refs[2:]
    (ag, m_right, m_left, ct, snd, recv, hid, outs, back, rs_right, rs_left, contrib, own,
     wi, wd, ag_s, ag_r, m_s, m_r, x_s, x_r, b_s, b_r, rs_s, rs_r, w_s, w_r, w_l) = refs

    z, x, c = lax.axis_index("ep"), lax.axis_index("dp"), lax.axis_index("tp")
    right, left = lax.rem(z + 1, nz), lax.rem(z + nz - 1, nz)
    peers = [lax.rem(x + k, nx) for k in range(nx)]

    def to(axis, index):
        return {axis: index}

    barrier = pltpu.get_barrier_semaphore()
    pl.semaphore_signal(barrier, inc=1, device_id=to("tp", 1 - c), device_id_type=MESH)
    for index in (right, left):
        pl.semaphore_signal(barrier, inc=1, device_id=to("ep", index), device_id_type=MESH)
    for k in range(1, nx):
        pl.semaphore_signal(barrier, inc=1, device_id=to("dp", peers[k]), device_id_type=MESH)
    pl.semaphore_wait(barrier, 2 + nx)

    def remote(src, dst, send, recv_sem, axis, index):
        return pltpu.make_async_remote_copy(
            src_ref=src, dst_ref=dst, send_sem=send, recv_sem=recv_sem,
            device_id=to(axis, index), device_id_type=MESH,
        )

    def cut(p, base=0):
        return pl.ds(base + p * pr, pr)

    def ring_copy(src, s, p, way):
        if way == 0:
            dst = ag.at[s, cut(p)]
        else:
            dst = ag.at[s, pl.ds(pl.multiple_of(jnp.where(s == steps, p * pr, tok + p * pr), pr), pr)]
        return remote(src, dst, ag_s.at[way, s, p], ag_r.at[way, s, p], "ep", (right, left)[way])

    def ring_block(s, p, way):
        if way == 0:
            return ag.at[s, cut(p)]
        return ag.at[s, cut(p, tok)]

    def meta_copy(src, s, way):
        return remote(src, (m_right, m_left)[way].at[s], m_s.at[way, s], m_r.at[way, s], "ep", (right, left)[way])

    for p in range(PIECES):
        for way in (0, 1):
            ring_copy(rows_ref.at[cut(p)], jnp.int32(1), p, way).start()
        if p == 0:
            for way in (0, 1):
                meta_copy(meta_ref, 1, way).start()

    mine = [
        pltpu.make_async_copy(w_in, wi.at[0], w_l.at[0]),
        pltpu.make_async_copy(w_down, wd.at[0], w_l.at[1]),
    ]
    other = [
        remote(w_in, wi.at[1], w_s.at[0], w_r.at[0], "tp", 1 - c),
        remote(w_down, wd.at[1], w_s.at[1], w_r.at[1], "tp", 1 - c),
    ]
    for k in (0, 1):
        other[k].start()
        mine[k].start()

    ag[steps, pl.ds(tok, tok)] = rows_ref[...]
    m_left[steps] = meta_ref[...]
    quiet = tok // 2
    rs_right[1, pl.ds(quiet, tok - quiet)] = jnp.zeros((tok - quiet, width), BF16)
    rs_left[1, pl.ds(0, quiet)] = jnp.zeros((quiet, width), BF16)

    lane = lax.broadcasted_iota(jnp.int32, (8, 2 * tok), 1)
    first = (z * nx).astype(F32)

    def select(s):
        info = jnp.concatenate([m_right[s][:, :tok], m_left[s][:, :tok]], axis=1)
        ids, gates = info[:top], info[top:]
        hits, values = [], []
        for k in range(nx):
            hit = ids == first + k
            hits.append(jnp.sum(jnp.where(hit, 1.0, 0.0), axis=0, keepdims=True))
            values.append(jnp.sum(jnp.where(hit, gates, 0.0), axis=0, keepdims=True))
        hit_all = jnp.concatenate(hits + [jnp.zeros((8 - nx, 2 * tok), F32)], axis=0)
        a = lax.broadcasted_iota(jnp.int32, (2 * tok, 2 * tok), 0)
        b = lax.broadcasted_iota(jnp.int32, (2 * tok, 2 * tok), 1)
        before = jnp.where((a < b) & ((a >= tok) == (b >= tok)), 1.0, 0.0).astype(BF16)
        rank = jnp.dot(hit_all.astype(BF16), before, preferred_element_type=F32)
        code = jnp.where(hit_all > 0.5, rank + jnp.where(lane >= tok, float(cap), 0.0), -1.0)
        place = lax.broadcasted_iota(jnp.int32, (rows, 2 * tok), 0).astype(F32)
        ones, weights = [], []
        for k in range(nx):
            pick = jnp.where(place == code[k:k + 1], 1.0, 0.0)
            ones.append(pick)
            weights.append(pick * values[k])
        pick = jnp.concatenate(ones, axis=0).astype(BF16)
        weight = jnp.concatenate(weights, axis=0)
        high = weight.astype(BF16)
        ct[s] = jnp.concatenate([high, (weight - high.astype(F32)).astype(BF16)], axis=1)
        chosen = jnp.dot(pick, ag[s], preferred_element_type=F32).astype(BF16)
        snd[s] = chosen.reshape(nx, rows, width)
        for k in range(1, nx):
            to_expert(s, k).start()
        recv[s, x] = snd[s, x]

    def to_expert(s, k):
        return remote(snd.at[s, peers[k]], recv.at[s, x], x_s.at[s, k], x_r.at[s, k], "dp", peers[k])

    def from_owner(s, k):
        source = lax.rem(x + nx - k, nx)
        return remote(snd.at[s, source], recv.at[s, source], x_s.at[s, k], x_r.at[s, k], "dp", peers[k])

    def to_owner(s, k):
        return remote(outs.at[s, peers[k]], back.at[s, x], b_s.at[s, k], b_r.at[s, k], "dp", peers[k])

    def from_expert(s, k):
        source = lax.rem(x + nx - k, nx)
        return remote(outs.at[s, source], back.at[s, source], b_s.at[s, k], b_r.at[s, k], "dp", peers[k])

    def hidden(s, h):
        got = recv[s].reshape(slab, width)
        both = jnp.dot(got, wi[h], preferred_element_type=F32)
        gate, up = both[:, :half_ff], both[:, half_ff:]
        hid[h] = (gate * (1.0 / (1.0 + jnp.exp(-gate))) * up).astype(BF16)

    def down(s):
        parts = [jnp.dot(hid[h], wd[h], preferred_element_type=F32).astype(BF16).astype(F32) for h in (0, 1)]
        outs[s] = (parts[0] + parts[1]).astype(BF16).reshape(nx, rows, width)
        back[s, x] = outs[s, x]

    def gather_step(s, carry):
        for p in range(PIECES):
            moving = s <= steps - 1
            here = [moving | ((s == steps) & (p < PIECES // 2)), moving | ((s == steps) & (p >= PIECES // 2))]
            onward = [(s < steps - 1) | ((s == steps - 1) & (p < PIECES // 2)),
                      (s < steps - 1) | ((s == steps - 1) & (p >= PIECES // 2))]
            for way in (0, 1):
                @pl.when(here[way])
                def _():
                    ring_copy(ring_block(1, p, way), s, p, way).wait_recv()

                @pl.when(onward[way])
                def _():
                    ring_copy(ring_block(s, p, way), s + 1, p, way).start()
            if p == 0:
                @pl.when(s <= steps)
                def _():
                    meta_copy(meta_ref, s, 0).wait_recv()

                @pl.when(moving)
                def _():
                    meta_copy(meta_ref, s, 1).wait_recv()
                    meta_copy(m_right.at[s], s + 1, 0).start()

                @pl.when(s < steps - 1)
                def _():
                    meta_copy(m_left.at[s], s + 1, 1).start()

                @pl.when((s >= 2) & (s <= steps + 1))
                def _():
                    select(s - 1)
            if p == 1:
                @pl.when(s == 3)
                def _():
                    for k in (0, 1):
                        mine[k].wait()
                        other[k].wait()

                @pl.when(s >= 3)
                def _():
                    for k in range(1, nx):
                        from_owner(s - 2, k).wait_recv()
                    hidden(s - 2, 0)
            if p == 2:
                @pl.when(s >= 3)
                def _():
                    hidden(s - 2, 1)
            if p == 3:
                @pl.when(s >= 3)
                def _():
                    down(s - 2)

                @pl.when(s >= steps + 1)
                def _():
                    for k in range(1, nx):
                        to_owner(s - 2, k).start()
        return carry

    lax.fori_loop(1, steps + 3, gather_step, 0)

    def return_rest(i, carry):
        for k in range(1, nx):
            to_owner(steps - 2 - i, k).start()
        return carry

    lax.fori_loop(0, steps - 2, return_rest, 0)

    def scatter_copy(src, j, p, way):
        dst = (rs_right, rs_left)[way].at[j, cut(p)]
        return remote(src, dst, rs_s.at[way, j, p], rs_r.at[way, j, p], "ep", (right, left)[way])

    def combine(s):
        for k in range(1, nx):
            from_expert(s, k).wait_recv()
        both = lax.dot_general(ct[s], back[s].reshape(slab, width), (((0,), (0,)), ((), ())),
                               preferred_element_type=F32)
        contrib[...] = both[:2 * tok] + both[2 * tok:]

    combine(steps)
    for p in range(PIECES):
        way = 0 if p < PIECES // 2 else 1
        buf = (rs_right, rs_left)[way]
        buf[0, cut(p)] = contrib[cut(p)].astype(BF16)
        scatter_copy(buf.at[0, cut(p)], 1, p, way).start()
    own[...] = contrib[pl.ds(tok, tok)]

    def scatter_step(j, carry):
        combine(steps - j)
        for p in range(PIECES):
            for way in (0, 1):
                buf = (rs_right, rs_left)[way]

                @pl.when((j >= 2) | ((p < PIECES // 2) == (way == 0)))
                def _():
                    scatter_copy(buf.at[0, cut(p)], j, p, way).wait_recv()

                part = contrib[cut(p, tok if way == 0 else 0)]
                buf[j, cut(p)] = (buf[j, cut(p)].astype(F32) + part).astype(BF16)
                scatter_copy(buf.at[j, cut(p)], j + 1, p, way).start()
        return carry

    lax.fori_loop(1, steps, scatter_step, 0)

    for p in range(PIECES):
        for way in (0, 1):
            buf = (rs_right, rs_left)[way]
            scatter_copy(buf.at[0, cut(p)], steps, p, way).wait_recv()
        total = own[cut(p)] + rs_right[steps, cut(p)].astype(F32) + rs_left[steps, cut(p)].astype(F32)
        mixed = (resid_ref[cut(p)].astype(F32) + total).astype(BF16)
        if with_norm:
            mixed_ref[cut(p)] = mixed
            wide = mixed.astype(F32)
            scale = lax.rsqrt(jnp.mean(wide * wide, axis=1, keepdims=True) + 1e-06)
            normed_ref[cut(p)] = (wide * scale * gain_ref[...]).astype(BF16)
        else:
            out_ref[cut(p)] = mixed

    def sent(s, carry):
        for p in range(PIECES):
            for way in (0, 1):
                @pl.when((s < steps) | ((p < PIECES // 2) == (way == 0)))
                def _():
                    ring_copy(ring_block(1, p, way), s, p, way).wait_send()

                @pl.when((s > 1) | ((p < PIECES // 2) == (way == 0)))
                def _():
                    scatter_copy((rs_right, rs_left)[way].at[0, cut(p)], s, p, way).wait_send()
        meta_copy(meta_ref, s, 0).wait_send()

        @pl.when(s < steps)
        def _():
            meta_copy(meta_ref, s, 1).wait_send()
        for k in range(1, nx):
            to_expert(s, k).wait_send()
            to_owner(s, k).wait_send()
        return carry

    lax.fori_loop(1, steps + 1, sent, 0)


def moe_layer(sizes, cap, with_norm, collective_id, rows_in, meta, w_in, w_down, extra):
    nz, nx = sizes
    tok, width = rows_in.shape
    half_ff = w_down.shape[0]
    top = meta.shape[0] // 2
    rows = -(-2 * cap // 16) * 16
    dims = (nz, nx, tok, width, half_ff, top, cap, rows)
    groups = nz // 2 + 1
    dma = pltpu.SemaphoreType.DMA
    vmem, hbm = pl.BlockSpec(memory_space=pltpu.VMEM), pl.BlockSpec(memory_space=pl.ANY)
    shape = jax.ShapeDtypeStruct((tok, width), BF16)
    scratch = [
        pltpu.VMEM((groups, 2 * tok, width), BF16),
        pltpu.VMEM((groups, *meta.shape), F32),
        pltpu.VMEM((groups, *meta.shape), F32),
        pltpu.VMEM((groups, nx * rows, 4 * tok), BF16),
        pltpu.VMEM((groups, nx, rows, width), BF16),
        pltpu.VMEM((groups, nx, rows, width), BF16),
        pltpu.VMEM((2, nx * rows, half_ff), BF16),
        pltpu.VMEM((groups, nx, rows, width), BF16),
        pltpu.VMEM((groups, nx, rows, width), BF16),
        pltpu.VMEM((groups, tok, width), BF16),
        pltpu.VMEM((groups, tok, width), BF16),
        pltpu.VMEM((2 * tok, width), F32),
        pltpu.VMEM((tok, width), F32),
        pltpu.VMEM((2, width, 2 * half_ff), BF16),
        pltpu.VMEM((2, half_ff, width), BF16),
        dma((2, groups, PIECES)),
        dma((2, groups, PIECES)),
        dma((2, groups)),
        dma((2, groups)),
        dma((groups, nx)),
        dma((groups, nx)),
        dma((groups, nx)),
        dma((groups, nx)),
        dma((2, groups, PIECES)),
        dma((2, groups, PIECES)),
        dma((2,)),
        dma((2,)),
        dma((2,)),
    ]
    return pl.pallas_call(
        functools.partial(layer_kernel, dims, with_norm),
        out_shape=(shape, shape) if with_norm else shape,
        in_specs=[vmem, vmem, hbm, hbm, vmem],
        out_specs=(vmem, vmem) if with_norm else vmem,
        scratch_shapes=scratch,
        compiler_params=pltpu.CompilerParams(
            collective_id=collective_id, has_side_effects=True, vmem_limit_bytes=60 * 1024 * 1024
        ),
        name="moe_norm" if with_norm else "moe_last",
    )(rows_in, meta, w_in, w_down, extra)


def routing(ids, gates):
    wide = jnp.concatenate([ids.T.astype(F32), gates.T], axis=0)
    return jnp.pad(wide, ((0, 0), (0, -wide.shape[1] % 128)))


def shards(sizes, tokens, experts_one, gates_one, w_in_one, w_down_one, norm_gain,
           experts_two, gates_two, placement_two, w_in_two, w_down_two):
    tok_rows, top_count = experts_one.shape
    expert_count = placement_two.shape[0]
    cap = capacity(tok_rows, top_count, expert_count)
    expert_range = jnp.arange(expert_count, dtype=jnp.int32)
    matches = experts_two[:, :, None] == expert_range[None, None, :]
    slots_two = jnp.sum(jnp.where(matches, placement_two[None, None, :], 0), axis=2)

    def flat(w):
        return w[0].reshape(w.shape[1], w.shape[2] * w.shape[3])

    mixed, normed = moe_layer(sizes, cap, True, 0, tokens, routing(experts_one, gates_one),
                              flat(w_in_one), w_down_one[0], norm_gain[None, :])
    return moe_layer(sizes, cap, False, 1, normed, routing(slots_two, gates_two),
                     flat(w_in_two), w_down_two[0], mixed)


def solution(mesh):
    own = P(("groups", "ep", "dp", "tp"), None)
    w_in, w_down = P(("ep", "dp"), None, None, "tp"), P(("ep", "dp"), "tp", None)
    in_specs = (own, own, own, w_in, w_down, P(), own, own, P(), w_in, w_down)
    sizes = (mesh.shape["ep"], mesh.shape["dp"])
    return jax.shard_map(functools.partial(shards, sizes), mesh=mesh, in_specs=in_specs, out_specs=own,
                         check_vma=False)
```

```python
import functools

import jax
import jax.numpy as jnp
from jax import lax
from jax.experimental import pallas as pl
from jax.experimental.pallas import tpu as pltpu
from jax.sharding import PartitionSpec as P

F32, BF16 = jnp.float32, jnp.bfloat16
MESH = pl.DeviceIdType.MESH
PIECES = 4
LAYERS = 2


def capacity(tok_rows, top_count, expert_count):
    return max(2, min(tok_rows, 5 * tok_rows * top_count // (4 * expert_count)))


def round_up(n, unit):
    return -(-n // unit) * unit


def kernel(dims, tok_ref, ids_one, gates_one, ids_two, gates_two, place_ref, gain_ref,
           w_in_one, w_down_one, w_in_two, w_down_two, out_ref,
           ag, m_right, m_left, ct, snd, recv, hid, outs, back, rs_right, rs_left, contrib, own,
           mixed, raw, wi, wd,
           ag_s, ag_r, m_s, m_r, x_s, x_r, b_s, b_r, rs_s, rs_r, w_s, w_r, w_l, w_free):
    nz, nx, tok, width, half_ff, top, cap, rows, few, experts = dims
    steps = nz // 2
    pr = tok // PIECES
    half = PIECES // 2
    slab = nx * rows
    w_in, w_down = (w_in_one, w_in_two), (w_down_one, w_down_two)

    z, x, c = lax.axis_index("ep"), lax.axis_index("dp"), lax.axis_index("tp")
    right, left = lax.rem(z + 1, nz), lax.rem(z + nz - 1, nz)
    peers = [lax.rem(x + k, nx) for k in range(nx)]
    sources = [lax.rem(x + nx - k, nx) for k in range(nx)]

    barrier = pltpu.get_barrier_semaphore()
    pl.semaphore_signal(barrier, inc=1, device_id={"tp": 1 - c}, device_id_type=MESH)
    for index in (right, left):
        pl.semaphore_signal(barrier, inc=1, device_id={"ep": index}, device_id_type=MESH)
    for k in range(1, nx):
        pl.semaphore_signal(barrier, inc=1, device_id={"dp": peers[k]}, device_id_type=MESH)
    pl.semaphore_wait(barrier, 2 + nx)

    def remote(src, dst, send, recv_sem, axis, index):
        return pltpu.make_async_remote_copy(
            src_ref=src, dst_ref=dst, send_sem=send, recv_sem=recv_sem,
            device_id={axis: index}, device_id_type=MESH,
        )

    def cut(p, base=0):
        return pl.ds(base + p * pr, pr)

    def ring_copy(l, src, s, p, way):
        if way == 0:
            dst = ag.at[l, s, cut(p)]
        else:
            dst = ag.at[l, s, pl.ds(pl.multiple_of(jnp.where(s == steps, p * pr, tok + p * pr), pr), pr)]
        return remote(src, dst, ag_s.at[l, way, s, p], ag_r.at[l, way, s, p], "ep", (right, left)[way])

    def ring_block(l, s, p, way):
        return ag.at[l, s, cut(p, 0 if way == 0 else tok)]

    def meta_copy(src, s, way):
        return remote(src, (m_right, m_left)[way].at[s], m_s.at[way, s], m_r.at[way, s], "ep", (right, left)[way])

    def begin(l, p):
        for way in (0, 1):
            ring_copy(l, ag.at[l, 0, cut(p)], jnp.int32(1), p, way).start()

    def x_copy(l, src, dst, sems, s, k, count):
        send, recv_sem = sems
        return remote(src.at[:count], dst.at[:count], send.at[l, s, k], recv_sem.at[l, s, k], "dp", peers[k])

    def by_size(s, act):
        @pl.when(s == steps)
        def _():
            act(few)

        @pl.when(s != steps)
        def _():
            act(rows)

    def to_expert(l, s, k, n):
        return x_copy(l, snd.at[s, peers[k]], recv.at[l, s, x], (x_s, x_r), s, k, n)

    def from_owner(l, s, k, n):
        return x_copy(l, snd.at[s, sources[k]], recv.at[l, s, sources[k]], (x_s, x_r), s, k, n)

    def to_owner(l, s, k, n):
        return x_copy(l, outs.at[s, peers[k]], back.at[l, s, x], (b_s, b_r), s, k, n)

    def from_expert(l, s, k, n):
        return x_copy(l, outs.at[s, sources[k]], back.at[l, s, sources[k]], (b_s, b_r), s, k, n)

    others = range(1, nx)
    lane = lax.broadcasted_iota(jnp.int32, (8, 2 * tok), 1)
    first = (z * nx).astype(F32)

    def select(l, s):
        at = pl.ds(0, top), pl.ds(top, top)
        info = [jnp.concatenate([m_right[s, a][:, l * tok:(l + 1) * tok], m_left[s, a][:, l * tok:(l + 1) * tok]], axis=1)
                for a in at]
        ids, gates = info
        hits, values = [], []
        for k in range(nx):
            hit = ids == first + k
            hits.append(jnp.sum(jnp.where(hit, 1.0, 0.0), axis=0, keepdims=True))
            values.append(jnp.sum(jnp.where(hit, gates, 0.0), axis=0, keepdims=True))
        hit_all = jnp.concatenate(hits + [jnp.zeros((8 - nx, 2 * tok), F32)], axis=0)
        a = lax.broadcasted_iota(jnp.int32, (2 * tok, 2 * tok), 0)
        b = lax.broadcasted_iota(jnp.int32, (2 * tok, 2 * tok), 1)
        before = jnp.where((a < b) & ((a >= tok) == (b >= tok)), 1.0, 0.0).astype(BF16)
        rank = jnp.dot(hit_all.astype(BF16), before, preferred_element_type=F32)
        code = jnp.where(hit_all > 0.5, rank + jnp.where(lane >= tok, float(cap), 0.0), -1.0)
        place = lax.broadcasted_iota(jnp.int32, (rows, 2 * tok), 0).astype(F32)
        ones, weights = [], []
        for k in range(nx):
            pick = jnp.where(place == code[k:k + 1], 1.0, 0.0)
            ones.append(pick)
            weights.append(pick * values[k])
        pick = jnp.concatenate(ones, axis=0).astype(BF16)
        weight = jnp.concatenate(weights, axis=0)
        high = weight.astype(BF16)
        ct[s] = jnp.concatenate([high, (weight - high.astype(F32)).astype(BF16)], axis=1)
        chosen = jnp.dot(pick, ag[l, s], preferred_element_type=F32).astype(BF16)
        for k in range(nx):
            snd[s, k] = chosen[k * rows:(k + 1) * rows]

        def send(n):
            for k in others:
                to_expert(l, s, k, n).start()

        by_size(s, send)
        recv[l, s, x] = snd[s, x]

    def await_rows(l, s):
        def act(n):
            for k in others:
                from_owner(l, s, k, n).wait_recv()

        by_size(s, act)

    def hidden(l, s, h):
        got = jnp.concatenate([recv[l, s, k] for k in range(nx)], axis=0)
        both = jnp.dot(got, wi[h], preferred_element_type=F32)
        gate, up = both[:, :half_ff], both[:, half_ff:]
        hid[h] = (gate * (1.0 / (1.0 + jnp.exp(-gate))) * up).astype(BF16)

    def down(l, s):
        parts = [jnp.dot(hid[h], wd[h], preferred_element_type=F32).astype(BF16).astype(F32) for h in (0, 1)]
        total = (parts[0] + parts[1]).astype(BF16)
        for k in range(nx):
            outs[s, k] = total[k * rows:(k + 1) * rows]
        back[l, s, x] = outs[s, x]

    def give_back(l, s):
        def act(n):
            for k in others:
                to_owner(l, s, k, n).start()

        by_size(s, act)

    def load_in(l):
        return pltpu.make_async_copy(w_in[l].at[0], raw, w_l.at[l, 0])

    def load_down(l):
        return pltpu.make_async_copy(w_down[l].at[0], wd.at[0], w_l.at[l, 1])

    def give_in(l):
        return remote(wi.at[0], wi.at[1], w_s.at[l, 0], w_r.at[l, 0], "tp", 1 - c)

    def give_down(l):
        return remote(w_down[l].at[0], wd.at[1], w_s.at[l, 1], w_r.at[l, 1], "tp", 1 - c)

    def sort_in(p):
        part = width // PIECES
        unit = min(64, part)

        def body(i, carry):
            at = pl.ds(pl.multiple_of(p * part + i * unit, unit), unit)
            wi[0, at, :half_ff] = raw[at, 0, :]
            wi[0, at, half_ff:] = raw[at, 1, :]
            return carry

        lax.fori_loop(0, part // unit, body, 0)

    def scatter_copy(l, src, j, p, way):
        dst = (rs_right, rs_left)[way].at[l, j, cut(p)]
        return remote(src, dst, rs_s.at[l, way, j, p], rs_r.at[l, way, j, p], "ep", (right, left)[way])

    def combine(l, s):
        def act(n):
            for k in others:
                from_expert(l, s, k, n).wait_recv()

        by_size(s, act)
        got = jnp.concatenate([back[l, s, k] for k in range(nx)], axis=0)
        both = lax.dot_general(ct[s], got, (((0,), (0,)), ((), ())), preferred_element_type=F32)
        contrib[...] = both[:2 * tok] + both[2 * tok:]

    def run_layer(l):
        def gather_step(s, carry):
            moving = s <= steps - 1
            for p in range(PIECES):
                for way in (0, 1):
                    mid = (p < half) == (way == 0)
                    here = (moving & (s >= 1)) | ((s == steps) & mid)
                    onward = ((s < steps - 1) & (s >= 1)) | ((s == steps - 1) & mid)

                    @pl.when(here)
                    def _():
                        ring_copy(l, ring_block(l, 1, p, way), s, p, way).wait_recv()

                    @pl.when(onward)
                    def _():
                        ring_copy(l, ring_block(l, s, p, way), s + 1, p, way).start()
                if p == 0:
                    if l == 0:
                        @pl.when((s >= 1) & (s <= steps))
                        def _():
                            meta_copy(m_right.at[0], s, 0).wait_recv()

                        @pl.when((s >= 1) & moving)
                        def _():
                            meta_copy(m_right.at[0], s, 1).wait_recv()
                            meta_copy(m_right.at[s], s + 1, 0).start()

                        @pl.when((s >= 1) & (s < steps - 1))
                        def _():
                            meta_copy(m_left.at[s], s + 1, 1).start()

                    @pl.when((s >= 1) & (s <= steps + 1))
                    def _():
                        select(l, s - 1)
                if p == 1:
                    @pl.when(s == 1)
                    def _():
                        if l > 0:
                            pl.semaphore_wait(w_free, 1)
                            give_down(l).start()
                        give_in(l).start()

                    @pl.when(s == 2)
                    def _():
                        load_down(l).wait()
                        give_in(l).wait()
                        give_down(l).wait()

                    @pl.when(s >= 2)
                    def _():
                        await_rows(l, s - 2)
                        hidden(l, s - 2, 0)
                if p == 2:
                    @pl.when(s >= 2)
                    def _():
                        hidden(l, s - 2, 1)
                if p == 3:
                    @pl.when(s >= 2)
                    def _():
                        down(l, s - 2)

                    @pl.when(s >= steps + 1)
                    def _():
                        give_back(l, s - 2)
                @pl.when(s == 0)
                def _():
                    if p == 0:
                        load_in(l).wait()
                    sort_in(p)
            return carry

        lax.fori_loop(0, steps + 3, gather_step, 0)

        if l + 1 < LAYERS:
            pl.semaphore_signal(w_free, inc=1, device_id={"tp": 1 - c}, device_id_type=MESH)
            load_in(l + 1).start()
            load_down(l + 1).start()

        def return_rest(i, carry):
            for k in others:
                to_owner(l, steps - 2 - i, k, rows).start()
            return carry

        lax.fori_loop(0, steps - 1, return_rest, 0)

        combine(l, steps)
        for p in range(PIECES):
            way = 0 if p < half else 1
            buf = (rs_right, rs_left)[way]
            buf[l, 0, cut(p)] = contrib[cut(p)].astype(BF16)
            scatter_copy(l, buf.at[l, 0, cut(p)], 1, p, way).start()

        def scatter_step(j, carry):
            combine(l, steps - j)
            for p in range(PIECES):
                for way in (0, 1):
                    buf = (rs_right, rs_left)[way]

                    @pl.when((j >= 2) | ((p < half) == (way == 0)))
                    def _():
                        scatter_copy(l, buf.at[l, 0, cut(p)], j, p, way).wait_recv()

                    part = contrib[cut(p, tok if way == 0 else 0)]
                    buf[l, j, cut(p)] = (buf[l, j, cut(p)].astype(F32) + part).astype(BF16)
                    scatter_copy(l, buf.at[l, j, cut(p)], j + 1, p, way).start()
            return carry

        lax.fori_loop(1, steps, scatter_step, 0)

        combine(l, 0)
        own[...] = contrib[:tok]
        for p in range(PIECES):
            for way in (0, 1):
                buf = (rs_right, rs_left)[way]
                scatter_copy(l, buf.at[l, 0, cut(p)], steps, p, way).wait_recv()
            total = own[cut(p)] + rs_right[l, steps, cut(p)].astype(F32) + rs_left[l, steps, cut(p)].astype(F32)
            before = tok_ref if l == 0 else mixed
            after = (before[cut(p)].astype(F32) + total).astype(BF16)
            if l + 1 < LAYERS:
                mixed[cut(p)] = after
                wide = after.astype(F32)
                scale = lax.rsqrt(jnp.mean(wide * wide, axis=1, keepdims=True) + 1e-06)
                ag[l + 1, 0, cut(p)] = (wide * scale * gain_ref[...]).astype(BF16)
                begin(l + 1, p)
            else:
                out_ref[cut(p)] = after

        def sent(s, carry):
            for p in range(PIECES):
                for way in (0, 1):
                    mid = (p < half) == (way == 0)

                    @pl.when((s < steps) | mid)
                    def _():
                        ring_copy(l, ring_block(l, 1, p, way), s, p, way).wait_send()

                    @pl.when((s > 1) | mid)
                    def _():
                        scatter_copy(l, (rs_right, rs_left)[way].at[l, 0, cut(p)], s, p, way).wait_send()
            if l == 0:
                meta_copy(m_right.at[0], s, 0).wait_send()

                @pl.when(s < steps)
                def _():
                    meta_copy(m_right.at[0], s, 1).wait_send()
            return carry

        lax.fori_loop(1, steps + 1, sent, 0)

        def x_sent(s, carry):
            def act(n):
                for k in others:
                    to_expert(l, s, k, n).wait_send()
                    to_owner(l, s, k, n).wait_send()

            by_size(s, act)
            return carry

        lax.fori_loop(0, steps + 1, x_sent, 0)

    load_in(0).start()
    load_down(0).start()
    give_down(0).start()
    ag[0, 0, pl.ds(0, tok)] = tok_ref[...]
    for p in range(PIECES):
        for way in (0, 1):
            ring_copy(0, tok_ref.at[cut(p)], jnp.int32(1), p, way).start()
        if p == 0:
            slots = jnp.zeros(ids_two.shape, jnp.int32)
            for e in range(experts):
                slots = jnp.where(ids_two[...] == e, place_ref[e], slots)
            m_right[0, pl.ds(0, top)] = jnp.concatenate([ids_one[...], slots], axis=1).astype(F32)
            m_right[0, pl.ds(top, top)] = jnp.concatenate([gates_one[...], gates_two[...]], axis=1)
            for way in (0, 1):
                meta_copy(m_right.at[0], 1, way).start()
    nobody = jnp.full(m_left.shape[1:], -1.0, F32)
    m_left[0] = nobody
    m_left[steps] = nobody
    for l in range(LAYERS):
        ag[l, 0, pl.ds(tok, tok)] = jnp.zeros((tok, width), BF16)
        ag[l, steps, pl.ds(tok, tok)] = jnp.zeros((tok, width), BF16)
        for p in range(half, PIECES):
            rs_right[l, 1, cut(p)] = jnp.zeros((pr, width), BF16)
        for p in range(half):
            rs_left[l, 1, cut(p)] = jnp.zeros((pr, width), BF16)
        for k in range(nx):
            recv[l, steps, k, pl.ds(few, rows - few)] = jnp.zeros((rows - few, width), BF16)
            back[l, steps, k, pl.ds(few, rows - few)] = jnp.zeros((rows - few, width), BF16)
    for l in range(LAYERS):
        run_layer(l)


def moe(sizes, cap, tokens, ids_one, gates_one, ids_two, gates_two, placement, gain, w_in_one, w_down_one, w_in_two, w_down_two):
    nz, nx = sizes
    tok, width = tokens.shape
    half_ff = w_down_one.shape[1]
    top = ids_one.shape[0]
    rows, few = round_up(2 * cap, 8), round_up(cap, 8)
    dims = (nz, nx, tok, width, half_ff, top, cap, rows, few, placement.shape[0])
    groups = nz // 2 + 1
    dma = pltpu.SemaphoreType.DMA
    vmem, hbm = pl.BlockSpec(memory_space=pltpu.VMEM), pl.BlockSpec(memory_space=pl.ANY)
    smem = pl.BlockSpec(memory_space=pltpu.SMEM)
    slots = (groups, nx, rows, width)
    scratch = [
        pltpu.VMEM((LAYERS, groups, 2 * tok, width), BF16),
        pltpu.VMEM((groups, 2 * top, LAYERS * tok), F32),
        pltpu.VMEM((groups, 2 * top, LAYERS * tok), F32),
        pltpu.VMEM((groups, nx * rows, 4 * tok), BF16),
        pltpu.VMEM(slots, BF16),
        pltpu.VMEM((LAYERS, *slots), BF16),
        pltpu.VMEM((2, nx * rows, half_ff), BF16),
        pltpu.VMEM(slots, BF16),
        pltpu.VMEM((LAYERS, *slots), BF16),
        pltpu.VMEM((LAYERS, groups, tok, width), BF16),
        pltpu.VMEM((LAYERS, groups, tok, width), BF16),
        pltpu.VMEM((2 * tok, width), F32),
        pltpu.VMEM((tok, width), F32),
        pltpu.VMEM((tok, width), BF16),
        pltpu.VMEM(w_in_one.shape[1:], BF16),
        pltpu.VMEM((2, width, 2 * half_ff), BF16),
        pltpu.VMEM((2, half_ff, width), BF16),
        dma((LAYERS, 2, groups, PIECES)),
        dma((LAYERS, 2, groups, PIECES)),
        dma((2, groups)),
        dma((2, groups)),
        dma((LAYERS, groups, nx)),
        dma((LAYERS, groups, nx)),
        dma((LAYERS, groups, nx)),
        dma((LAYERS, groups, nx)),
        dma((LAYERS, 2, groups, PIECES)),
        dma((LAYERS, 2, groups, PIECES)),
        dma((LAYERS, 2)),
        dma((LAYERS, 2)),
        dma((LAYERS, 2)),
        pltpu.SemaphoreType.REGULAR,
    ]
    return pl.pallas_call(
        functools.partial(kernel, dims),
        out_shape=jax.ShapeDtypeStruct((tok, width), BF16),
        in_specs=[vmem] * 5 + [smem, vmem] + [hbm] * 4,
        out_specs=vmem,
        scratch_shapes=scratch,
        compiler_params=pltpu.CompilerParams(
            collective_id=0, has_side_effects=True, vmem_limit_bytes=63 * 1024 * 1024
        ),
        name="moe_pair",
    )(tokens, ids_one, gates_one, ids_two, gates_two, placement, gain, w_in_one, w_down_one, w_in_two, w_down_two)


def shards(sizes, tokens, experts_one, gates_one, w_in_one, w_down_one, norm_gain,
           experts_two, gates_two, placement_two, w_in_two, w_down_two):
    tok_rows, top_count = experts_one.shape
    cap = capacity(tok_rows, top_count, placement_two.shape[0])
    return moe(sizes, cap, tokens, experts_one.T, gates_one.T, experts_two.T, gates_two.T, placement_two,
               norm_gain[None, :], w_in_one, w_down_one, w_in_two, w_down_two)


def solution(mesh):
    own = P(("groups", "ep", "dp", "tp"), None)
    w_in, w_down = P(("ep", "dp"), None, None, "tp"), P(("ep", "dp"), "tp", None)
    in_specs = (own, own, own, w_in, w_down, P(), own, own, P(), w_in, w_down)
    sizes = (mesh.shape["ep"], mesh.shape["dp"])
    return jax.shard_map(functools.partial(shards, sizes), mesh=mesh, in_specs=in_specs, out_specs=own,
                         check_vma=False)
```

```python
import functools

import jax
import jax.numpy as jnp
from jax import lax
from jax.experimental import pallas as pl
from jax.experimental.pallas import tpu as pltpu
from jax.sharding import PartitionSpec as P

F32, BF16 = jnp.float32, jnp.bfloat16
MESH = pl.DeviceIdType.MESH
PIECES = 4
LAYERS = 2
HEAD_START = 4


def capacity(tok_rows, top_count, expert_count):
    return max(2, min(tok_rows, 5 * tok_rows * top_count // (4 * expert_count)))


def round_up(n, unit):
    return -(-n // unit) * unit


def kernel(dims, tok_ref, ids_one, gates_one, ids_two, gates_two, place_ref, gain_ref,
           w_in_one, w_down_one, w_in_two, w_down_two, out_ref,
           ag, m_right, m_left, ct, snd, recv, hid, outs, back, rs_right, rs_left, contrib, own,
           mixed, raw, wi, wd,
           ag_s, ag_r, m_s, m_r, x_s, x_r, b_s, b_r, rs_s, rs_r, w_s, w_r, w_l, w_free, go):
    nz, nx, tok, width, half_ff, top, cap, rows, few, experts = dims
    steps = nz // 2
    pr = tok // PIECES
    half = PIECES // 2
    sort_steps = min(4, steps - 1)
    head_start = min(HEAD_START, steps)
    slab = nx * rows
    w_in, w_down = (w_in_one, w_in_two), (w_down_one, w_down_two)

    z, x, c = lax.axis_index("ep"), lax.axis_index("dp"), lax.axis_index("tp")
    right, left = lax.rem(z + 1, nz), lax.rem(z + nz - 1, nz)
    peers = [lax.rem(x + k, nx) for k in range(nx)]
    sources = [lax.rem(x + nx - k, nx) for k in range(nx)]

    barrier = pltpu.get_barrier_semaphore()
    pl.semaphore_signal(barrier, inc=1, device_id={"tp": 1 - c}, device_id_type=MESH)
    for index in (right, left):
        pl.semaphore_signal(barrier, inc=1, device_id={"ep": index}, device_id_type=MESH)
    for k in range(1, nx):
        pl.semaphore_signal(barrier, inc=1, device_id={"dp": peers[k]}, device_id_type=MESH)
    pl.semaphore_wait(barrier, 2 + nx)

    def remote(src, dst, send, recv_sem, axis, index):
        return pltpu.make_async_remote_copy(
            src_ref=src, dst_ref=dst, send_sem=send, recv_sem=recv_sem,
            device_id={axis: index}, device_id_type=MESH,
        )

    def cut(p, base=0):
        return pl.ds(base + p * pr, pr)

    def ring_copy(l, src, s, p, way):
        if way == 0:
            dst = ag.at[l, s, cut(p)]
        else:
            dst = ag.at[l, s, pl.ds(pl.multiple_of(jnp.where(s == steps, p * pr, tok + p * pr), pr), pr)]
        return remote(src, dst, ag_s.at[l, way, s, p], ag_r.at[l, way, s, p], "ep", (right, left)[way])

    def ring_block(l, s, p, way):
        return ag.at[l, s, cut(p, 0 if way == 0 else tok)]

    def meta_copy(src, s, way):
        return remote(src, (m_right, m_left)[way].at[s], m_s.at[way, s], m_r.at[way, s], "ep", (right, left)[way])

    def begin(l, p):
        for way in (0, 1):
            ring_copy(l, ag.at[l, 0, cut(p)], jnp.int32(1), p, way).start()

    def x_copy(l, src, dst, sems, s, k, count):
        send, recv_sem = sems
        return remote(src.at[:count], dst.at[:count], send.at[l, s, k], recv_sem.at[l, s, k], "dp", peers[k])

    def by_size(s, act):
        @pl.when(s == steps)
        def _():
            act(few)

        @pl.when(s != steps)
        def _():
            act(rows)

    def to_expert(l, s, k, n):
        return x_copy(l, snd.at[s, peers[k]], recv.at[l, s, x], (x_s, x_r), s, k, n)

    def from_owner(l, s, k, n):
        return x_copy(l, snd.at[s, sources[k]], recv.at[l, s, sources[k]], (x_s, x_r), s, k, n)

    def to_owner(l, s, k, n):
        return x_copy(l, outs.at[s, peers[k]], back.at[l, s, x], (b_s, b_r), s, k, n)

    def from_expert(l, s, k, n):
        return x_copy(l, outs.at[s, sources[k]], back.at[l, s, sources[k]], (b_s, b_r), s, k, n)

    others = range(1, nx)
    lane = lax.broadcasted_iota(jnp.int32, (8, 2 * tok), 1)
    first = (z * nx).astype(F32)

    def select(l, s):
        at = pl.ds(0, top), pl.ds(top, top)
        info = [jnp.concatenate([m_right[s, a][:, l * tok:(l + 1) * tok], m_left[s, a][:, l * tok:(l + 1) * tok]], axis=1)
                for a in at]
        ids, gates = info
        hits, values = [], []
        for k in range(nx):
            hit = ids == first + k
            hits.append(jnp.sum(jnp.where(hit, 1.0, 0.0), axis=0, keepdims=True))
            values.append(jnp.sum(jnp.where(hit, gates, 0.0), axis=0, keepdims=True))
        hit_all = jnp.concatenate(hits + [jnp.zeros((8 - nx, 2 * tok), F32)], axis=0)
        a = lax.broadcasted_iota(jnp.int32, (2 * tok, 2 * tok), 0)
        b = lax.broadcasted_iota(jnp.int32, (2 * tok, 2 * tok), 1)
        before = jnp.where((a < b) & ((a >= tok) == (b >= tok)), 1.0, 0.0).astype(BF16)
        rank = jnp.dot(hit_all.astype(BF16), before, preferred_element_type=F32)
        code = jnp.where(hit_all > 0.5, rank + jnp.where(lane >= tok, float(cap), 0.0), -1.0)
        place = lax.broadcasted_iota(jnp.int32, (rows, 2 * tok), 0).astype(F32)
        ones, weights = [], []
        for k in range(nx):
            pick = jnp.where(place == code[k:k + 1], 1.0, 0.0)
            ones.append(pick)
            weights.append(pick * values[k])
        pick = jnp.concatenate(ones, axis=0).astype(BF16)
        weight = jnp.concatenate(weights, axis=0)
        high = weight.astype(BF16)
        ct[s] = jnp.concatenate([high, (weight - high.astype(F32)).astype(BF16)], axis=1)
        chosen = jnp.dot(pick, ag[l, s], preferred_element_type=F32).astype(BF16)
        for k in range(nx):
            snd[s, k] = chosen[k * rows:(k + 1) * rows]

        def send(n):
            for k in others:
                to_expert(l, s, k, n).start()

        by_size(s, send)
        recv[l, s, x] = snd[s, x]

    def await_rows(l, s):
        def act(n):
            for k in others:
                from_owner(l, s, k, n).wait_recv()

        by_size(s, act)

    def hidden(l, s, h):
        got = jnp.concatenate([recv[l, s, k] for k in range(nx)], axis=0)
        both = jnp.dot(got, wi[h], preferred_element_type=F32)
        gate, up = both[:, :half_ff], both[:, half_ff:]
        hid[lax.rem(s, 2), h] = (gate * (1.0 / (1.0 + jnp.exp(-gate))) * up).astype(BF16)

    def down(l, s):
        parts = [jnp.dot(hid[lax.rem(s, 2), h], wd[h], preferred_element_type=F32).astype(BF16).astype(F32) for h in (0, 1)]
        total = (parts[0] + parts[1]).astype(BF16)
        for k in range(nx):
            outs[s, k] = total[k * rows:(k + 1) * rows]
        back[l, s, x] = outs[s, x]

    def give_back(l, s):
        def act(n):
            for k in others:
                to_owner(l, s, k, n).start()

        by_size(s, act)

    def load_in(l):
        return pltpu.make_async_copy(w_in[l].at[0], raw, w_l.at[l, 0])

    def load_down(l):
        return pltpu.make_async_copy(w_down[l].at[0], wd.at[0], w_l.at[l, 1])

    def give_in(l):
        return remote(wi.at[0], wi.at[1], w_s.at[l, 0], w_r.at[l, 0], "tp", 1 - c)

    def give_down(l):
        return remote(w_down[l].at[0], wd.at[1], w_s.at[l, 1], w_r.at[l, 1], "tp", 1 - c)

    def sort_in(i):
        unit = width // (sort_steps * PIECES)
        at = pl.ds(pl.multiple_of(i * unit, unit), unit)
        wi[0, at, :half_ff] = raw[at, 0, :]
        wi[0, at, half_ff:] = raw[at, 1, :]

    def sort_all(l):
        load_in(l).wait()

        def body(i, carry):
            sort_in(i)
            return carry

        lax.fori_loop(0, sort_steps * PIECES, body, 0)

    def scatter_copy(l, src, j, p, way):
        dst = (rs_right, rs_left)[way].at[l, j, cut(p)]
        return remote(src, dst, rs_s.at[l, way, j, p], rs_r.at[l, way, j, p], "ep", (right, left)[way])

    def combine(l, s):
        def act(n):
            for k in others:
                from_expert(l, s, k, n).wait_recv()

        by_size(s, act)
        got = jnp.concatenate([back[l, s, k] for k in range(nx)], axis=0)
        both = lax.dot_general(ct[s], got, (((0,), (0,)), ((), ())), preferred_element_type=F32)
        contrib[...] = both[:2 * tok] + both[2 * tok:]

    def run_layer(l):
        ready = jnp.where(c == 1, 2, sort_steps + 1) if l == 0 else min(3, steps)

        def bound(s):
            at = jnp.where(s == steps + 1, steps, s)
            return jnp.where(at <= ready, 0, jnp.minimum(2 * (at - ready), at - 2))

        def each_group(s, act):
            def body(g, carry):
                act(g)
                return carry

            lax.fori_loop(bound(s), bound(s + 1), body, 0)

        def first_half(g):
            await_rows(l, g)
            hidden(l, g, 0)

        def gather_step(s, carry):
            moving = s <= steps - 1
            for p in range(PIECES):
                for way in (0, 1):
                    mid = (p < half) == (way == 0)
                    here = (moving & (s >= 1)) | ((s == steps) & mid)
                    onward = ((s < steps - 1) & (s >= 1)) | ((s == steps - 1) & mid)

                    @pl.when(here)
                    def _():
                        ring_copy(l, ring_block(l, 1, p, way), s, p, way).wait_recv()

                    @pl.when(onward)
                    def _():
                        ring_copy(l, ring_block(l, s, p, way), s + 1, p, way).start()
                if p == 0:
                    if l == 0:
                        @pl.when((s >= 1) & (s <= steps))
                        def _():
                            meta_copy(m_right.at[0], s, 0).wait_recv()

                        @pl.when((s >= 1) & moving)
                        def _():
                            meta_copy(m_right.at[0], s, 1).wait_recv()
                            meta_copy(m_right.at[s], s + 1, 0).start()

                        @pl.when((s >= 1) & (s < steps - 1))
                        def _():
                            meta_copy(m_left.at[s], s + 1, 1).start()

                        @pl.when((s == head_start) & (c == 0))
                        def _():
                            pl.semaphore_signal(go, inc=1, device_id={"tp": 1 - c}, device_id_type=MESH)

                        @pl.when((s == sort_steps) & (c == 0))
                        def _():
                            give_in(0).start()
                            load_in(1).start()
                    else:
                        @pl.when((s == 1) & (c == 0))
                        def _():
                            pl.semaphore_wait(w_free, 1)
                            give_down(l).start()
                            give_in(l).start()

                    @pl.when((s >= 1) & (s <= steps + 1))
                    def _():
                        select(l, s - 1)
                if p == 1:
                    @pl.when(s == ready)
                    def _():
                        load_down(l).wait()
                        give_in(l).wait()
                        give_down(l).wait()

                    each_group(s, first_half)
                if p == 2:
                    each_group(s, lambda g: hidden(l, g, 1))
                if p == 3:
                    each_group(s, lambda g: down(l, g))
                if l == 0:
                    @pl.when((s < sort_steps) & (c == 0))
                    def _():
                        if p == 0:
                            @pl.when(s == 0)
                            def _():
                                load_in(0).wait()
                        sort_in(s * PIECES + p)
            return carry

        lax.fori_loop(0, steps + 3, gather_step, 0)

        def return_rows(i, carry):
            give_back(l, steps - i)
            return carry

        lax.fori_loop(0, steps + 1, return_rows, 0)

        if l + 1 < LAYERS:
            pl.semaphore_signal(w_free, inc=1, device_id={"tp": 1 - c}, device_id_type=MESH)
            load_down(l + 1).start()
            sort_all(l + 1)

            @pl.when(c == 1)
            def _():
                pl.semaphore_wait(w_free, 1)
                give_down(l + 1).start()
                give_in(l + 1).start()

        combine(l, steps)
        for p in range(PIECES):
            way = 0 if p < half else 1
            buf = (rs_right, rs_left)[way]
            buf[l, 0, cut(p)] = contrib[cut(p)].astype(BF16)
            scatter_copy(l, buf.at[l, 0, cut(p)], 1, p, way).start()

        def scatter_step(j, carry):
            combine(l, steps - j)
            for p in range(PIECES):
                for way in (0, 1):
                    buf = (rs_right, rs_left)[way]

                    @pl.when((j >= 2) | ((p < half) == (way == 0)))
                    def _():
                        scatter_copy(l, buf.at[l, 0, cut(p)], j, p, way).wait_recv()

                    part = contrib[cut(p, tok if way == 0 else 0)]
                    buf[l, j, cut(p)] = (buf[l, j, cut(p)].astype(F32) + part).astype(BF16)
                    scatter_copy(l, buf.at[l, j, cut(p)], j + 1, p, way).start()
            return carry

        lax.fori_loop(1, steps, scatter_step, 0)

        combine(l, 0)
        own[...] = contrib[:tok]
        for p in range(PIECES):
            for way in (0, 1):
                buf = (rs_right, rs_left)[way]
                scatter_copy(l, buf.at[l, 0, cut(p)], steps, p, way).wait_recv()
            total = own[cut(p)] + rs_right[l, steps, cut(p)].astype(F32) + rs_left[l, steps, cut(p)].astype(F32)
            before = tok_ref if l == 0 else mixed
            after = (before[cut(p)].astype(F32) + total).astype(BF16)
            if l + 1 < LAYERS:
                mixed[cut(p)] = after
                wide = after.astype(F32)
                scale = lax.rsqrt(jnp.mean(wide * wide, axis=1, keepdims=True) + 1e-06)
                ag[l + 1, 0, cut(p)] = (wide * scale * gain_ref[...]).astype(BF16)
                begin(l + 1, p)
            else:
                out_ref[cut(p)] = after

        def sent(s, carry):
            for p in range(PIECES):
                for way in (0, 1):
                    mid = (p < half) == (way == 0)

                    @pl.when((s < steps) | mid)
                    def _():
                        ring_copy(l, ring_block(l, 1, p, way), s, p, way).wait_send()

                    @pl.when((s > 1) | mid)
                    def _():
                        scatter_copy(l, (rs_right, rs_left)[way].at[l, 0, cut(p)], s, p, way).wait_send()
            if l == 0:
                meta_copy(m_right.at[0], s, 0).wait_send()

                @pl.when(s < steps)
                def _():
                    meta_copy(m_right.at[0], s, 1).wait_send()
            return carry

        lax.fori_loop(1, steps + 1, sent, 0)

        def x_sent(s, carry):
            def act(n):
                for k in others:
                    to_expert(l, s, k, n).wait_send()
                    to_owner(l, s, k, n).wait_send()

            by_size(s, act)
            return carry

        lax.fori_loop(0, steps + 1, x_sent, 0)

    load_in(0).start()
    load_down(0).start()
    give_down(0).start()
    ag[0, 0, pl.ds(0, tok)] = tok_ref[...]

    @pl.when(c == 0)
    def _():
        for p in range(PIECES):
            begin(0, p)

    slots = jnp.zeros(ids_two.shape, jnp.int32)
    for e in range(experts):
        slots = jnp.where(ids_two[...] == e, place_ref[e], slots)
    m_right[0, pl.ds(0, top)] = jnp.concatenate([ids_one[...], slots], axis=1).astype(F32)
    m_right[0, pl.ds(top, top)] = jnp.concatenate([gates_one[...], gates_two[...]], axis=1)
    for way in (0, 1):
        meta_copy(m_right.at[0], 1, way).start()
    nobody = jnp.full(m_left.shape[1:], -1.0, F32)
    m_left[0] = nobody
    m_left[steps] = nobody
    for l in range(LAYERS):
        ag[l, 0, pl.ds(tok, tok)] = jnp.zeros((tok, width), BF16)
        ag[l, steps, pl.ds(tok, tok)] = jnp.zeros((tok, width), BF16)
        for p in range(half, PIECES):
            rs_right[l, 1, cut(p)] = jnp.zeros((pr, width), BF16)
        for p in range(half):
            rs_left[l, 1, cut(p)] = jnp.zeros((pr, width), BF16)
        for k in range(nx):
            recv[l, steps, k, pl.ds(few, rows - few)] = jnp.zeros((rows - few, width), BF16)
            back[l, steps, k, pl.ds(few, rows - few)] = jnp.zeros((rows - few, width), BF16)

    @pl.when(c == 1)
    def _():
        sort_all(0)
        give_in(0).start()
        load_in(1).start()
        pl.semaphore_wait(go, 1)
        for p in range(PIECES):
            begin(0, p)

    for l in range(LAYERS):
        run_layer(l)


def moe(sizes, cap, tokens, ids_one, gates_one, ids_two, gates_two, placement, gain, w_in_one, w_down_one, w_in_two, w_down_two):
    nz, nx = sizes
    tok, width = tokens.shape
    half_ff = w_down_one.shape[1]
    top = ids_one.shape[0]
    rows, few = round_up(2 * cap, 8), round_up(cap, 8)
    dims = (nz, nx, tok, width, half_ff, top, cap, rows, few, placement.shape[0])
    groups = nz // 2 + 1
    dma = pltpu.SemaphoreType.DMA
    vmem, hbm = pl.BlockSpec(memory_space=pltpu.VMEM), pl.BlockSpec(memory_space=pl.ANY)
    smem = pl.BlockSpec(memory_space=pltpu.SMEM)
    slots = (groups, nx, rows, width)
    scratch = [
        pltpu.VMEM((LAYERS, groups, 2 * tok, width), BF16),
        pltpu.VMEM((groups, 2 * top, LAYERS * tok), F32),
        pltpu.VMEM((groups, 2 * top, LAYERS * tok), F32),
        pltpu.VMEM((groups, nx * rows, 4 * tok), BF16),
        pltpu.VMEM(slots, BF16),
        pltpu.VMEM((LAYERS, *slots), BF16),
        pltpu.VMEM((2, 2, nx * rows, half_ff), BF16),
        pltpu.VMEM(slots, BF16),
        pltpu.VMEM((LAYERS, *slots), BF16),
        pltpu.VMEM((LAYERS, groups, tok, width), BF16),
        pltpu.VMEM((LAYERS, groups, tok, width), BF16),
        pltpu.VMEM((2 * tok, width), F32),
        pltpu.VMEM((tok, width), F32),
        pltpu.VMEM((tok, width), BF16),
        pltpu.VMEM(w_in_one.shape[1:], BF16),
        pltpu.VMEM((2, width, 2 * half_ff), BF16),
        pltpu.VMEM((2, half_ff, width), BF16),
        dma((LAYERS, 2, groups, PIECES)),
        dma((LAYERS, 2, groups, PIECES)),
        dma((2, groups)),
        dma((2, groups)),
        dma((LAYERS, groups, nx)),
        dma((LAYERS, groups, nx)),
        dma((LAYERS, groups, nx)),
        dma((LAYERS, groups, nx)),
        dma((LAYERS, 2, groups, PIECES)),
        dma((LAYERS, 2, groups, PIECES)),
        dma((LAYERS, 2)),
        dma((LAYERS, 2)),
        dma((LAYERS, 2)),
        pltpu.SemaphoreType.REGULAR,
        pltpu.SemaphoreType.REGULAR,
    ]
    return pl.pallas_call(
        functools.partial(kernel, dims),
        out_shape=jax.ShapeDtypeStruct((tok, width), BF16),
        in_specs=[vmem] * 5 + [smem, vmem] + [hbm] * 4,
        out_specs=vmem,
        scratch_shapes=scratch,
        compiler_params=pltpu.CompilerParams(
            collective_id=0, has_side_effects=True, vmem_limit_bytes=63 * 1024 * 1024
        ),
        name="moe_pair",
    )(tokens, ids_one, gates_one, ids_two, gates_two, placement, gain, w_in_one, w_down_one, w_in_two, w_down_two)


def shards(sizes, tokens, experts_one, gates_one, w_in_one, w_down_one, norm_gain,
           experts_two, gates_two, placement_two, w_in_two, w_down_two):
    tok_rows, top_count = experts_one.shape
    cap = capacity(tok_rows, top_count, placement_two.shape[0])
    return moe(sizes, cap, tokens, experts_one.T, gates_one.T, experts_two.T, gates_two.T, placement_two,
               norm_gain[None, :], w_in_one, w_down_one, w_in_two, w_down_two)


def solution(mesh):
    own = P(("groups", "ep", "dp", "tp"), None)
    w_in, w_down = P(("ep", "dp"), None, None, "tp"), P(("ep", "dp"), "tp", None)
    in_specs = (own, own, own, w_in, w_down, P(), own, own, P(), w_in, w_down)
    sizes = (mesh.shape["ep"], mesh.shape["dp"])
    return jax.shard_map(functools.partial(shards, sizes), mesh=mesh, in_specs=in_specs, out_specs=own,
                         check_vma=False)
```

```python
import functools

import jax
import jax.numpy as jnp
from jax import lax
from jax.experimental import pallas as pl
from jax.experimental.pallas import tpu as pltpu
from jax.sharding import PartitionSpec as P

F32, BF16 = jnp.float32, jnp.bfloat16
MESH = pl.DeviceIdType.MESH
PIECES = 4
LAYERS = 2
HEAD_START = 3
FIRST = 0


def capacity(tok_rows, top_count, expert_count):
    return max(2, min(tok_rows, 5 * tok_rows * top_count // (4 * expert_count)))


def round_up(n, unit):
    return -(-n // unit) * unit


def kernel(dims, tok_ref, ids_one, gates_one, ids_two, gates_two, place_ref, gain_ref,
           w_in_one, w_down_one, w_in_two, w_down_two, out_ref,
           ag, m_right, m_left, ct, snd, recv, hid, outs, back, rs_right, rs_left, contrib, own,
           mixed, raw, wi, wd,
           ag_s, ag_r, m_s, m_r, x_s, x_r, b_s, b_r, rs_s, rs_r, w_s, w_r, w_l, w_free, go):
    nz, nx, tok, width, half_ff, top, cap, rows, few, experts = dims
    steps = nz // 2
    pr = tok // PIECES
    half = PIECES // 2
    sort_steps = min(4, steps - 1)
    head_start = min(HEAD_START, steps)
    slab = nx * rows
    w_in, w_down = (w_in_one, w_in_two), (w_down_one, w_down_two)

    z, x, c = lax.axis_index("ep"), lax.axis_index("dp"), lax.axis_index("tp")
    right, left = lax.rem(z + 1, nz), lax.rem(z + nz - 1, nz)
    peers = [lax.rem(x + k, nx) for k in range(nx)]

    barrier = pltpu.get_barrier_semaphore()
    pl.semaphore_signal(barrier, inc=1, device_id={"tp": 1 - c}, device_id_type=MESH)
    for index in (right, left):
        pl.semaphore_signal(barrier, inc=1, device_id={"ep": index}, device_id_type=MESH)
    for k in range(1, nx):
        pl.semaphore_signal(barrier, inc=1, device_id={"dp": peers[k]}, device_id_type=MESH)
    pl.semaphore_wait(barrier, 2 + nx)

    def remote(src, dst, send, recv_sem, axis, index):
        return pltpu.make_async_remote_copy(
            src_ref=src, dst_ref=dst, send_sem=send, recv_sem=recv_sem,
            device_id={axis: index}, device_id_type=MESH,
        )

    def cut(p, base=0):
        return pl.ds(base + p * pr, pr)

    def ring_copy(l, src, s, p, way):
        if way == 0:
            dst = ag.at[l, s, cut(p)]
        else:
            dst = ag.at[l, s, pl.ds(pl.multiple_of(jnp.where(s == steps, p * pr, tok + p * pr), pr), pr)]
        return remote(src, dst, ag_s.at[way, s], ag_r.at[way, s, p], "ep", (right, left)[way])

    def ring_block(l, s, p, way):
        return ag.at[l, s, cut(p, 0 if way == 0 else tok)]

    def ring_sent(l, s, way, count):
        return remote(ag.at[l, 1, :count], ag.at[l, 1, :count], ag_s.at[way, s], ag_r.at[way, s, 0], "ep", (right, left)[way])

    def scatter_block(l, j, way, count):
        buf = (rs_right, rs_left)[way]
        return remote(buf.at[l, 1, :count], buf.at[l, 1, :count], rs_s.at[way, j], rs_r.at[way, j, 0], "ep", (right, left)[way])

    def meta_copy(src, s, way):
        return remote(src, (m_right, m_left)[way].at[s], m_s.at[way], m_r.at[way, s], "ep", (right, left)[way])

    def begin(l, p):
        for way in (0, 1):
            ring_copy(l, ag.at[l, 0, cut(p)], jnp.int32(1), p, way).start()

    def x_copy(src, dst, sems, s, k, count):
        return remote(src.at[:count], dst.at[:count], sems[0].at[s], sems[1].at[s], "dp", peers[k])

    def x_all(l, sems, s, count):
        return remote(snd.at[s, :nx - 1, :count], recv.at[l, s, :nx - 1, :count], sems[0].at[s], sems[1].at[s], "dp", peers[1])

    def by_size(s, act):
        @pl.when(s == steps)
        def _():
            act(few)

        @pl.when(s != steps)
        def _():
            act(rows)

    def to_expert(l, s, k, n):
        return x_copy(snd.at[s, peers[k]], recv.at[l, s, x], (x_s, x_r), s, k, n)

    def to_owner(l, s, k, n):
        return x_copy(outs.at[s, peers[k]], back.at[l, s, x], (b_s, b_r), s, k, n)

    others = range(1, nx)
    lane = lax.broadcasted_iota(jnp.int32, (8, 2 * tok), 1)
    first = (z * nx).astype(F32)

    def select(l, s):
        at = pl.ds(0, top), pl.ds(top, top)
        info = [jnp.concatenate([m_right[s, a][:, l * tok:(l + 1) * tok], m_left[s, a][:, l * tok:(l + 1) * tok]], axis=1)
                for a in at]
        ids, gates = info
        hits, values = [], []
        for k in range(nx):
            hit = ids == first + k
            hits.append(jnp.sum(jnp.where(hit, 1.0, 0.0), axis=0, keepdims=True))
            values.append(jnp.sum(jnp.where(hit, gates, 0.0), axis=0, keepdims=True))
        hit_all = jnp.concatenate(hits + [jnp.zeros((8 - nx, 2 * tok), F32)], axis=0)
        a = lax.broadcasted_iota(jnp.int32, (2 * tok, 2 * tok), 0)
        b = lax.broadcasted_iota(jnp.int32, (2 * tok, 2 * tok), 1)
        before = jnp.where((a < b) & ((a >= tok) == (b >= tok)), 1.0, 0.0).astype(BF16)
        rank = jnp.dot(hit_all.astype(BF16), before, preferred_element_type=F32)
        code = jnp.where(hit_all > 0.5, rank + jnp.where(lane >= tok, float(cap), 0.0), -1.0)
        place = lax.broadcasted_iota(jnp.int32, (rows, 2 * tok), 0).astype(F32)
        ones, weights = [], []
        for k in range(nx):
            pick = jnp.where(place == code[k:k + 1], 1.0, 0.0)
            ones.append(pick)
            weights.append(pick * values[k])
        pick = jnp.concatenate(ones, axis=0).astype(BF16)
        weight = jnp.concatenate(weights, axis=0)
        high = weight.astype(BF16)
        ct[s] = jnp.concatenate([high, (weight - high.astype(F32)).astype(BF16)], axis=1)
        chosen = jnp.dot(pick, ag[l, s], preferred_element_type=F32).astype(BF16)
        for k in range(nx):
            snd[s, k] = chosen[k * rows:(k + 1) * rows]

        def send(n):
            for k in others:
                to_expert(l, s, k, n).start()

        by_size(s, send)
        recv[l, s, x] = snd[s, x]

    def await_rows(l, s):
        by_size(s, lambda n: x_all(l, (x_s, x_r), s, n).wait_recv())

    def hidden(l, s, h):
        got = jnp.concatenate([recv[l, s, k] for k in range(nx)], axis=0)
        both = jnp.dot(got, wi[h], preferred_element_type=F32)
        gate, up = both[:, :half_ff], both[:, half_ff:]
        hid[lax.rem(s, 2), h] = (gate * (1.0 / (1.0 + jnp.exp(-gate))) * up).astype(BF16)

    def down(l, s):
        parts = [jnp.dot(hid[lax.rem(s, 2), h], wd[h], preferred_element_type=F32).astype(BF16).astype(F32) for h in (0, 1)]
        total = (parts[0] + parts[1]).astype(BF16)
        for k in range(nx):
            outs[s, k] = total[k * rows:(k + 1) * rows]
        back[l, s, x] = outs[s, x]

    def give_back(l, s):
        def act(n):
            for k in others:
                to_owner(l, s, k, n).start()

        by_size(s, act)

    def load_in(l):
        return pltpu.make_async_copy(w_in[l].at[0], raw, w_l.at[0])

    def load_down(l):
        return pltpu.make_async_copy(w_down[l].at[0], wd.at[0], w_l.at[1])

    def give_in(l):
        return remote(wi.at[0], wi.at[1], w_s.at[0], w_r.at[0], "tp", 1 - c)

    def give_down(l):
        return remote(w_down[l].at[0], wd.at[1], w_s.at[1], w_r.at[1], "tp", 1 - c)

    def sort_in(i):
        unit = width // (sort_steps * PIECES)
        at = pl.ds(pl.multiple_of(i * unit, unit), unit)
        wi[0, at, :half_ff] = raw[at, 0, :]
        wi[0, at, half_ff:] = raw[at, 1, :]

    def sort_all(l):
        load_in(l).wait()

        def body(i, carry):
            sort_in(i)
            return carry

        lax.fori_loop(0, sort_steps * PIECES, body, 0)

    def scatter_copy(l, src, j, p, way):
        dst = (rs_right, rs_left)[way].at[l, j, cut(p)]
        return remote(src, dst, rs_s.at[way, j], rs_r.at[way, j, p], "ep", (right, left)[way])

    def combine(l, s):
        by_size(s, lambda n: x_all(l, (b_s, b_r), s, n).wait_recv())
        got = jnp.concatenate([back[l, s, k] for k in range(nx)], axis=0)
        both = lax.dot_general(ct[s], got, (((0,), (0,)), ((), ())), preferred_element_type=F32)
        contrib[...] = both[:2 * tok] + both[2 * tok:]

    def run_layer(l):
        ready = jnp.where(c != FIRST, 2, sort_steps + 1) if l == 0 else min(3, steps)

        def bound(s):
            at = jnp.where(s == steps + 1, steps, s)
            return jnp.where(at <= ready, 0, jnp.minimum(2 * (at - ready), at - 2))

        def each_group(s, act):
            def body(g, carry):
                act(g)
                return carry

            lax.fori_loop(bound(s), bound(s + 1), body, 0)

        def first_half(g):
            await_rows(l, g)
            hidden(l, g, 0)

        def gather_step(s, carry):
            moving = s <= steps - 1
            for p in range(PIECES):
                for way in (0, 1):
                    mid = (p < half) == (way == 0)
                    here = (moving & (s >= 1)) | ((s == steps) & mid)
                    onward = ((s < steps - 1) & (s >= 1)) | ((s == steps - 1) & mid)

                    @pl.when(here)
                    def _():
                        ring_copy(l, ring_block(l, 1, p, way), s, p, way).wait_recv()

                    @pl.when(onward)
                    def _():
                        ring_copy(l, ring_block(l, s, p, way), s + 1, p, way).start()
                if p == 0:
                    if l == 0:
                        @pl.when((s == head_start) & (c == FIRST))
                        def _():
                            pl.semaphore_signal(go, inc=1, device_id={"tp": 1 - c}, device_id_type=MESH)

                        @pl.when((s == sort_steps) & (c == FIRST))
                        def _():
                            give_in(0).start()
                            load_in(1).start()
                    else:
                        @pl.when((s == 1) & (c == FIRST))
                        def _():
                            pl.semaphore_wait(w_free, 1)
                            give_down(l).start()
                            give_in(l).start()

                    @pl.when((s >= 1) & (s <= steps + 1))
                    def _():
                        select(l, s - 1)
                if p == 1:
                    @pl.when(s == ready)
                    def _():
                        load_down(l).wait()
                        give_in(l).wait()
                        give_down(l).wait()

                    each_group(s, first_half)
                if p == 2:
                    each_group(s, lambda g: hidden(l, g, 1))
                if p == 3:
                    if l == 0:
                        @pl.when((s >= 1) & (s <= steps))
                        def _():
                            meta_copy(m_right.at[0], s, 0).wait_recv()

                        @pl.when((s >= 1) & moving)
                        def _():
                            meta_copy(m_right.at[0], s, 1).wait_recv()
                            meta_copy(m_right.at[s], s + 1, 0).start()

                        @pl.when((s >= 1) & (s < steps - 1))
                        def _():
                            meta_copy(m_left.at[s], s + 1, 1).start()

                    each_group(s, lambda g: down(l, g))
                if l == 0:
                    @pl.when((s < sort_steps) & (c == FIRST))
                    def _():
                        if p == 0:
                            @pl.when(s == 0)
                            def _():
                                load_in(0).wait()
                        sort_in(s * PIECES + p)
            return carry

        lax.fori_loop(0, steps + 3, gather_step, 0)

        def return_rows(i, carry):
            give_back(l, steps - i)
            return carry

        lax.fori_loop(0, steps + 1, return_rows, 0)

        def gathered(s, carry):
            for way in (0, 1):
                ring_sent(l, s, way, tok).wait_send()
            return carry

        def chosen_sent(s, carry):
            by_size(s, lambda n: x_all(l, (x_s, x_r), s, n).wait_send())
            return carry

        lax.fori_loop(1, steps, gathered, 0)
        for way in (0, 1):
            ring_sent(l, steps, way, tok // 2).wait_send()
        lax.fori_loop(0, steps + 1, chosen_sent, 0)
        if l == 0:
            remote(m_right.at[:steps], m_right.at[:steps], m_s.at[0], m_r.at[0, 1], "ep", right).wait_send()
            remote(m_left.at[:steps - 1], m_left.at[:steps - 1], m_s.at[1], m_r.at[1, 1], "ep", left).wait_send()

        if l + 1 < LAYERS:
            pl.semaphore_signal(w_free, inc=1, device_id={"tp": 1 - c}, device_id_type=MESH)
            load_down(l + 1).start()

        combine(l, steps)
        for p in range(PIECES):
            way = 0 if p < half else 1
            buf = (rs_right, rs_left)[way]
            buf[l, 0, cut(p)] = contrib[cut(p)].astype(BF16)
            scatter_copy(l, buf.at[l, 0, cut(p)], 1, p, way).start()

        def scatter_step(j, carry):
            combine(l, steps - j)
            for p in range(PIECES):
                if l + 1 < LAYERS:
                    @pl.when(j <= sort_steps)
                    def _():
                        if p == 0:
                            @pl.when(j == 1)
                            def _():
                                load_in(l + 1).wait()
                        sort_in((j - 1) * PIECES + p)

                    if p == PIECES - 1:
                        @pl.when((j == sort_steps) & (c != FIRST))
                        def _():
                            pl.semaphore_wait(w_free, 1)
                            give_down(l + 1).start()
                            give_in(l + 1).start()
                for way in (0, 1):
                    buf = (rs_right, rs_left)[way]

                    @pl.when((j >= 2) | ((p < half) == (way == 0)))
                    def _():
                        scatter_copy(l, buf.at[l, 0, cut(p)], j, p, way).wait_recv()

                    part = contrib[cut(p, tok if way == 0 else 0)]
                    buf[l, j, cut(p)] = (buf[l, j, cut(p)].astype(F32) + part).astype(BF16)
                    scatter_copy(l, buf.at[l, j, cut(p)], j + 1, p, way).start()
            return carry

        lax.fori_loop(1, steps, scatter_step, 0)

        combine(l, 0)
        own[...] = contrib[:tok]
        for p in range(PIECES):
            for way in (0, 1):
                buf = (rs_right, rs_left)[way]
                scatter_copy(l, buf.at[l, 0, cut(p)], steps, p, way).wait_recv()
            total = own[cut(p)] + rs_right[l, steps, cut(p)].astype(F32) + rs_left[l, steps, cut(p)].astype(F32)
            before = tok_ref if l == 0 else mixed
            after = (before[cut(p)].astype(F32) + total).astype(BF16)
            if l + 1 < LAYERS:
                mixed[cut(p)] = after
                wide = after.astype(F32)
                scale = lax.rsqrt(jnp.mean(wide * wide, axis=1, keepdims=True) + 1e-06)
                ag[l + 1, 0, cut(p)] = (wide * scale * gain_ref[...]).astype(BF16)
                begin(l + 1, p)
            else:
                out_ref[cut(p)] = after

        def scattered(j, carry):
            for way in (0, 1):
                scatter_block(l, j, way, tok).wait_send()
            return carry

        for way in (0, 1):
            scatter_block(l, 1, way, tok // 2).wait_send()
        lax.fori_loop(2, steps + 1, scattered, 0)

        def returned(s, carry):
            by_size(s, lambda n: x_all(l, (b_s, b_r), s, n).wait_send())
            return carry

        lax.fori_loop(0, steps + 1, returned, 0)

    load_in(0).start()
    load_down(0).start()
    give_down(0).start()
    ag[0, 0, pl.ds(0, tok)] = tok_ref[...]

    @pl.when(c == FIRST)
    def _():
        for p in range(PIECES):
            begin(0, p)

    slots = jnp.zeros(ids_two.shape, jnp.int32)
    for e in range(experts):
        slots = jnp.where(ids_two[...] == e, place_ref[e], slots)
    m_right[0, pl.ds(0, top)] = jnp.concatenate([ids_one[...], slots], axis=1).astype(F32)
    m_right[0, pl.ds(top, top)] = jnp.concatenate([gates_one[...], gates_two[...]], axis=1)
    for way in (0, 1):
        meta_copy(m_right.at[0], 1, way).start()
    nobody = jnp.full(m_left.shape[1:], -1.0, F32)
    m_left[0] = nobody
    m_left[steps] = nobody
    for l in range(LAYERS):
        ag[l, 0, pl.ds(tok, tok)] = jnp.zeros((tok, width), BF16)
        ag[l, steps, pl.ds(tok, tok)] = jnp.zeros((tok, width), BF16)
        for p in range(half, PIECES):
            rs_right[l, 1, cut(p)] = jnp.zeros((pr, width), BF16)
        for p in range(half):
            rs_left[l, 1, cut(p)] = jnp.zeros((pr, width), BF16)
        for k in range(nx):
            recv[l, steps, k, pl.ds(few, rows - few)] = jnp.zeros((rows - few, width), BF16)
            back[l, steps, k, pl.ds(few, rows - few)] = jnp.zeros((rows - few, width), BF16)

    @pl.when(c != FIRST)
    def _():
        sort_all(0)
        give_in(0).start()
        load_in(1).start()
        pl.semaphore_wait(go, 1)
        for p in range(PIECES):
            begin(0, p)

    for l in range(LAYERS):
        run_layer(l)


def moe(sizes, cap, tokens, ids_one, gates_one, ids_two, gates_two, placement, gain, w_in_one, w_down_one, w_in_two, w_down_two):
    nz, nx = sizes
    tok, width = tokens.shape
    half_ff = w_down_one.shape[1]
    top = ids_one.shape[0]
    rows, few = round_up(2 * cap, 8), round_up(cap, 8)
    dims = (nz, nx, tok, width, half_ff, top, cap, rows, few, placement.shape[0])
    groups = nz // 2 + 1
    dma = pltpu.SemaphoreType.DMA
    vmem, hbm = pl.BlockSpec(memory_space=pltpu.VMEM), pl.BlockSpec(memory_space=pl.ANY)
    smem = pl.BlockSpec(memory_space=pltpu.SMEM)
    slots = (groups, nx, rows, width)
    scratch = [
        pltpu.VMEM((LAYERS, groups, 2 * tok, width), BF16),
        pltpu.VMEM((groups, 2 * top, LAYERS * tok), F32),
        pltpu.VMEM((groups, 2 * top, LAYERS * tok), F32),
        pltpu.VMEM((groups, nx * rows, 4 * tok), BF16),
        pltpu.VMEM(slots, BF16),
        pltpu.VMEM((LAYERS, *slots), BF16),
        pltpu.VMEM((2, 2, nx * rows, half_ff), BF16),
        pltpu.VMEM(slots, BF16),
        pltpu.VMEM((LAYERS, *slots), BF16),
        pltpu.VMEM((LAYERS, groups, tok, width), BF16),
        pltpu.VMEM((LAYERS, groups, tok, width), BF16),
        pltpu.VMEM((2 * tok, width), F32),
        pltpu.VMEM((tok, width), F32),
        pltpu.VMEM((tok, width), BF16),
        pltpu.VMEM(w_in_one.shape[1:], BF16),
        pltpu.VMEM((2, width, 2 * half_ff), BF16),
        pltpu.VMEM((2, half_ff, width), BF16),
        dma((2, groups)),
        dma((2, groups, PIECES)),
        dma((2,)),
        dma((2, groups)),
        dma((groups,)),
        dma((groups,)),
        dma((groups,)),
        dma((groups,)),
        dma((2, groups)),
        dma((2, groups, PIECES)),
        dma((2,)),
        dma((2,)),
        dma((2,)),
        pltpu.SemaphoreType.REGULAR,
        pltpu.SemaphoreType.REGULAR,
    ]
    return pl.pallas_call(
        functools.partial(kernel, dims),
        out_shape=jax.ShapeDtypeStruct((tok, width), BF16),
        in_specs=[vmem] * 5 + [smem, vmem] + [hbm] * 4,
        out_specs=vmem,
        scratch_shapes=scratch,
        compiler_params=pltpu.CompilerParams(
            collective_id=0, has_side_effects=True, vmem_limit_bytes=63 * 1024 * 1024
        ),
        name="moe_pair",
    )(tokens, ids_one, gates_one, ids_two, gates_two, placement, gain, w_in_one, w_down_one, w_in_two, w_down_two)


def shards(sizes, tokens, experts_one, gates_one, w_in_one, w_down_one, norm_gain,
           experts_two, gates_two, placement_two, w_in_two, w_down_two):
    tok_rows, top_count = experts_one.shape
    cap = capacity(tok_rows, top_count, placement_two.shape[0])
    return moe(sizes, cap, tokens, experts_one.T, gates_one.T, experts_two.T, gates_two.T, placement_two,
               norm_gain[None, :], w_in_one, w_down_one, w_in_two, w_down_two)


def solution(mesh):
    own = P(("groups", "ep", "dp", "tp"), None)
    w_in, w_down = P(("ep", "dp"), None, None, "tp"), P(("ep", "dp"), "tp", None)
    in_specs = (own, own, own, w_in, w_down, P(), own, own, P(), w_in, w_down)
    sizes = (mesh.shape["ep"], mesh.shape["dp"])
    return jax.shard_map(functools.partial(shards, sizes), mesh=mesh, in_specs=in_specs, out_specs=own,
                         check_vma=False)
```
